8 devices in a mesh: rep: 2 (over y, z), dp: 4 (over x, core).
Axes of the slice: x: 2, y: 2, z: 1, core: 2. Of those that a mesh axis runs over, the one named last changes fastest.
Arguments:
- x: bfloat16 [8, 2048, 1024], P(('rep', 'dp')), parts along dimension 0
- dy: bfloat16 [8, 2048, 1024], P(('rep', 'dp')), parts along dimension 0
- w_gate: bfloat16 [2, 1024, 3200], replicated
- w_up: bfloat16 [2, 1024, 3200], replicated
- w_down: bfloat16 [2, 3200, 1024], replicated
- m_w_gate: float32 [2, 1024, 3200], P(None, 'dp')
- m_w_up: float32 [2, 1024, 3200], P(None, 'dp')
- m_w_down: float32 [2, 3200, 1024], P(None, 'dp')
- v_w_gate: float32 [2, 1024, 3200], P(None, 'dp')
- v_w_up: float32 [2, 1024, 3200], P(None, 'dp')
- v_w_down: float32 [2, 3200, 1024], P(None, 'dp')
Outputs:
- output 1: bfloat16 [4, 1024, 3200], P('rep'), parts along dimension 0
- output 2: bfloat16 [4, 1024, 3200], P('rep'), parts along dimension 0
- output 3: bfloat16 [4, 3200, 1024], P('rep'), parts along dimension 0
- output 4: float32 [4, 1024, 3200], P('rep', 'dp'), parts along dimension 0
- output 5: float32 [4, 1024, 3200], P('rep', 'dp'), parts along dimension 0
- output 6: float32 [4, 3200, 1024], P('rep', 'dp'), parts along dimension 0
- output 7: float32 [4, 1024, 3200], P('rep', 'dp'), parts along dimension 0
- output 8: float32 [4, 1024, 3200], P('rep', 'dp'), parts along dimension 0
- output 9: float32 [4, 3200, 1024], P('rep', 'dp'), parts along dimension 0
There are 2 independent parts. The reference program is written for one: setup_inputs(seed, part) draws one part's arguments, and reference() takes and returns one part's arrays. A program takes and returns all parts, laid end to end along the dimension named above; an argument that names none is the same for every part.
All inputs are finite; a program needn't handle non-finite values.
Results may differ from the reference program's by a relative error of at most 0.0228.
Values are sent between devices in bfloat16 or wider.
A program may use at most 2 GiB of HBM per device.

```python
import jax
import jax.numpy as jnp
from jax import lax

SEQUENCES = 4
TOKENS = 2048
D = 1024
FF = 3200
LAYERS = 2
NAMES = ("w_gate", "w_up", "w_down")
SHAPES = {"w_gate": (LAYERS, D, FF), "w_up": (LAYERS, D, FF), "w_down": (LAYERS, FF, D)}


def bump(key, n, height):
    away = (jnp.arange(n, dtype=jnp.int32) - jax.random.randint(key, (), 0, n, jnp.int32)) % n
    return jnp.where(away < n // 8, height, 1.0)


def together(key, own, strength):
    shared = jax.random.normal(key, own.shape[1:], jnp.float32)
    return (own + strength * shared) * lax.rsqrt(1 + strength * strength)


def setup_inputs(seed: int = 0, part: int = 0) -> dict:
    kx, kdy, ka, kb, kz, kf, kh, kl, *keys = jax.random.split(jax.random.key(seed), 8 + 3 * len(NAMES))
    kx, kdy, ka, kb = (jax.random.fold_in(k, part) for k in (kx, kdy, ka, kb))
    kw, km, kv = (keys[i::3] for i in range(3))
    shape = (SEQUENCES, TOKENS, D)
    much_x, much_dy = jax.random.uniform(kz, (2,), jnp.float32, 0.0, 1.0)
    loud = 2.0 ** jax.random.uniform(jax.random.fold_in(kz, 1), (), jnp.float32, -1.0, 2.0)
    layers = 2.0 ** jax.random.uniform(kl, (LAYERS, 1, 1), jnp.float32, -1.0, 1.0)
    x = together(ka, jax.random.normal(kx, shape, jnp.float32), much_x) * bump(kf, D, 4.0)
    dy = together(kb, jax.random.normal(kdy, shape, jnp.float32), much_dy)
    drawn = {"x": x.astype(jnp.bfloat16), "dy": (loud * dy * (SEQUENCES * TOKENS) ** -0.5).astype(jnp.bfloat16)}
    for key, name in zip(kw, NAMES, strict=True):
        w = jax.random.normal(key, SHAPES[name], jnp.float32) * SHAPES[name][1] ** -0.5
        drawn[name] = (w * {"w_gate": 1.0, "w_up": bump(kh, FF, 4.0), "w_down": layers}[name]).astype(jnp.bfloat16)
    for key, name in zip(km, NAMES, strict=True):
        drawn[f"m_{name}"] = 0.1 * jax.random.normal(key, SHAPES[name], jnp.float32)
    for key, name in zip(kv, NAMES, strict=True):
        drawn[f"v_{name}"] = jax.random.uniform(key, SHAPES[name], jnp.float32, 0.005, 0.015)
    return drawn


def matmul(a, w):
    return jnp.dot(a, w, preferred_element_type=jnp.float32).astype(jnp.bfloat16)


def normed(h):
    wide = h.astype(jnp.float32)
    scale = lax.rsqrt(jnp.mean(wide**2, -1, keepdims=True) + 1e-6)
    return (wide * scale).astype(jnp.bfloat16)


def layer(h, w):
    a = normed(h)
    gate = jnp.dot(a, w["w_gate"], preferred_element_type=jnp.float32)
    up = jnp.dot(a, w["w_up"], preferred_element_type=jnp.float32)
    return h + matmul((jax.nn.silu(gate) * up).astype(jnp.bfloat16), w["w_down"])


def adamw(w, m, v, g):
    m = 0.9 * m + 0.1 * g
    v = 0.95 * v + 0.05 * g * g
    step = m * lax.rsqrt(v + 1e-8) + 0.1 * w
    return (w - 0.02 * step).astype(jnp.bfloat16), m, v


def stack(weights, h):
    return lax.scan(lambda h, w: (layer(h, w), None), h, weights)[0]


def reference(x, dy, w_gate, w_up, w_down, m_w_gate, m_w_up, m_w_down, v_w_gate, v_w_up, v_w_down):
    weights = dict(zip(NAMES, (w_gate, w_up, w_down), strict=True))

    def take(so_far, sequence):
        h, by_y = sequence
        _, back = jax.vjp(lambda w: stack(w, h), weights)
        return jax.tree.map(lambda total, term: total + term.astype(jnp.float32), so_far, back(by_y)[0]), None

    none_yet = {name: jnp.zeros(w.shape, jnp.float32) for name, w in weights.items()}
    by_weights, _ = lax.scan(take, none_yet, (x, dy))
    gradients = [by_weights[name].astype(jnp.bfloat16).astype(jnp.float32) for name in NAMES]
    new = [
        adamw(w.astype(jnp.float32), m, v, g)
        for w, m, v, g in zip((w_gate, w_up, w_down), (m_w_gate, m_w_up, m_w_down), (v_w_gate, v_w_up, v_w_down), gradients, strict=True)
    ]
    return tuple(one[which] for which in range(3) for one in new)
```

```python
import functools

import jax
import jax.numpy as jnp
from jax import lax
from jax.experimental import pallas as pl
from jax.experimental.pallas import tpu as pltpu
from jax.sharding import PartitionSpec as P

F32, BF16 = jnp.float32, jnp.bfloat16
CORES = [(0, 1), (1, 0), (2, 3), (3, 2)]
CHIPS = [(0, 2), (2, 0), (1, 3), (3, 1)]
T, D, F, C = 2048, 1024, 3200, 640
ROWS = 512
VMEM = 60 * 1024 * 1024
ME, PARTNER, ACROSS, DIAGONAL, MINE, OTHERS = 0, 1, 2, 3, 4, 9


def nn(a, b):
    return lax.dot_general(a, b, (((1,), (0,)), ((), ())), preferred_element_type=F32)


def nt(a, b):
    return lax.dot_general(a, b, (((1,), (1,)), ((), ())), preferred_element_type=F32)


def tn(a, b):
    return lax.dot_general(a, b, (((0,), (0,)), ((), ())), preferred_element_type=F32)


def normed(h):
    wide = h.astype(F32)
    return (wide * lax.rsqrt(jnp.mean(wide**2, -1, keepdims=True) + 1e-6)).astype(BF16)


def norm_back(h, da):
    wide = h.astype(F32)
    scale = lax.rsqrt(jnp.mean(wide**2, -1, keepdims=True) + 1e-6)
    da = da.astype(BF16).astype(F32)
    inner = jnp.mean(da * wide, -1, keepdims=True)
    return (scale * da - wide * (scale * scale * scale * inner)).astype(BF16)


def act_back(gate, up, dact):
    d = dact.astype(BF16).astype(F32)
    s = jax.nn.sigmoid(gate)
    silu = gate * s
    return (d * up * (s + silu * (1.0 - s))).astype(BF16), (d * silu).astype(BF16)


def over_tokens(body):
    @pl.loop(0, T // ROWS)
    def _(i):
        body(pl.ds(pl.multiple_of(i * ROWS, ROWS), ROWS))


def call(kernel, scalars, grid, ins, outs, scratch, name, flops, aliases=None):
    arrays = [a for a, _ in ins]
    moved = sum(a.size * a.dtype.itemsize for a in arrays)
    return pl.pallas_call(
        kernel,
        grid_spec=pltpu.PrefetchScalarGridSpec(
            num_scalar_prefetch=1, grid=(grid,), in_specs=[s for _, s in ins], out_specs=[s for _, s in outs], scratch_shapes=scratch
        ),
        out_shape=[s for s, _ in outs],
        input_output_aliases={k + 1: v for k, v in (aliases or {}).items()},
        compiler_params=pltpu.CompilerParams(dimension_semantics=("arbitrary",), vmem_limit_bytes=VMEM),
        cost_estimate=pl.CostEstimate(flops=int(flops), bytes_accessed=int(moved), transcendentals=0),
        name=name,
    )(scalars, *arrays)


def whole(shape):
    return pl.BlockSpec(shape, lambda j, s: (0,) * len(shape), pipeline_mode=pl.Buffered(1))


def shape(dims, dtype):
    return jax.ShapeDtypeStruct(dims, dtype)


MATMUL = 2 * T * D * F
ANY = pl.BlockSpec(memory_space=pl.ANY)


def forward(scalars, h, wg, wu, wd, layer):
    def kernel(s, h_ref, g_ref, u_ref, d_ref, a_out, out, total):
        j = pl.program_id(0)

        @pl.when(j == 0)
        def _():
            def body(t):
                a_out[t, :] = normed(h_ref[t, :])

            over_tokens(body)

        def body(t):
            a = a_out[t, :]
            gate, up = nn(a, g_ref[0]), nn(a, u_ref[0])
            part = nn((jax.nn.silu(gate) * up).astype(BF16), d_ref[0])

            @pl.when(j == 0)
            def _():
                total[t, :] = part

            @pl.when(j > 0)
            def _():
                total[t, :] += part

            @pl.when(j == F // C - 1)
            def _():
                out[t, :] = h_ref[t, :] + total[t, :].astype(BF16)

        over_tokens(body)

    return call(
        kernel, scalars, F // C,
        [(h, whole((T, D)))]
        + [(w, pl.BlockSpec((1, D, C), lambda j, s: (layer, 0, j))) for w in (wg, wu)]
        + [(wd, pl.BlockSpec((1, C, D), lambda j, s: (layer, j, 0)))],
        [(shape((T, D), BF16), whole((T, D)))] * 2,
        [pltpu.VMEM((T, D), F32)], "forward", 3 * MATMUL,
    )


def first_down(scalars, h, dy, wg, wu, layer, first, count):
    def kernel(s, h_ref, dy_ref, g_ref, u_ref, a_out, gate_out, up_out, gd_out, act):
        @pl.when(pl.program_id(0) == 0)
        def _():
            def body(t):
                a_out[t, :] = normed(h_ref[t, :])

            over_tokens(body)

        def body(t):
            a = a_out[t, :]
            gate, up = nn(a, g_ref[0]), nn(a, u_ref[0])
            gate_out[t, :] = gate
            up_out[t, :] = up
            act[t, :] = (jax.nn.silu(gate) * up).astype(BF16)

        over_tokens(body)
        gd_out[...] = tn(act[...], dy_ref[...]).astype(BF16)

    return call(
        kernel, scalars, count,
        [(h, whole((T, D))), (dy, whole((T, D)))]
        + [(w, pl.BlockSpec((1, D, C), lambda j, s: (layer, 0, s[MINE + first + j]))) for w in (wg, wu)],
        [(shape((T, D), BF16), whole((T, D)))]
        + [(shape((T, count * C), F32), pl.BlockSpec((T, C), lambda j, s: (0, j)))] * 2
        + [(shape((F, D), BF16), pl.BlockSpec((C, D), lambda j, s: (s[MINE + first + j], 0)))],
        [pltpu.VMEM((T, C), BF16)], "first_down", 3 * MATMUL * count * C // F,
    )


def sent_rows(a_refs, dg, du, outs):
    for which, a_ref in enumerate(a_refs):
        outs[which][...] = tn(a_ref[...], dg[...]).astype(BF16)
        outs[2 + which][...] = tn(a_ref[...], du[...]).astype(BF16)


def columns_of(a, which):
    return a, pl.BlockSpec((T, D // 4), lambda j, s: (0, s[which]), pipeline_mode=pl.Buffered(1))


def first_back(scalars, a, dy, gate, up, wd, layer, first, count):
    def kernel(s, dy_ref, gate_ref, up_ref, d_ref, a0, a1, dg_out, du_out, *outs):
        def body(t):
            dg, du = act_back(gate_ref[t, :], up_ref[t, :], nt(dy_ref[t, :], d_ref[0]))
            dg_out[t, :] = dg
            du_out[t, :] = du

        over_tokens(body)
        sent_rows((a0, a1), dg_out, du_out, outs)

    return call(
        kernel, scalars, count,
        [(dy, whole((T, D)))]
        + [(t, pl.BlockSpec((T, C), lambda j, s: (0, j))) for t in (gate, up)]
        + [(wd, pl.BlockSpec((1, C, D), lambda j, s: (layer, s[MINE + first + j], 0)))]
        + [columns_of(a, DIAGONAL), columns_of(a, ACROSS)],
        [(shape((T, F), BF16), pl.BlockSpec((T, C), lambda j, s: (0, s[MINE + first + j])))] * 2
        + [(shape((D // 4, count * C), BF16), pl.BlockSpec((D // 4, C), lambda j, s: (0, j)))] * 4,
        [], "first_back", 2 * MATMUL * count * C // F,
    )


def chunks_back(scalars, a, dh, wg, wu, wd, layer, first, count, filled=None):
    def kernel(s, a_ref, dh_ref, g_ref, u_ref, d_ref, a0, a1, *rest):
        dg_out, du_out, gd_out, *outs, act = rest[3:] if filled else rest

        def body(t):
            a, dh = a_ref[t, :], dh_ref[t, :]
            gate, up = nn(a, g_ref[0]), nn(a, u_ref[0])
            act[t, :] = (jax.nn.silu(gate) * up).astype(BF16)
            dg, du = act_back(gate, up, nt(dh, d_ref[0]))
            dg_out[t, :] = dg
            du_out[t, :] = du

        over_tokens(body)
        gd_out[...] = tn(act[...], dh_ref[...]).astype(BF16)
        sent_rows((a0, a1), dg_out, du_out, outs)

    return call(
        kernel, scalars, count,
        [(a, whole((T, D))), (dh, whole((T, D)))]
        + [(w, pl.BlockSpec((1, D, C), lambda j, s: (layer, 0, s[MINE + first + j]))) for w in (wg, wu)]
        + [(wd, pl.BlockSpec((1, C, D), lambda j, s: (layer, s[MINE + first + j], 0)))]
        + [columns_of(a, DIAGONAL), columns_of(a, ACROSS)]
        + [(t, ANY) for t in filled or ()],
        [(shape((T, F), BF16), pl.BlockSpec((T, C), lambda j, s: (0, s[MINE + first + j])))] * 2
        + [(shape((F, D), BF16), pl.BlockSpec((C, D), lambda j, s: (s[MINE + first + j], 0)))]
        + [(shape((D // 4, count * C), BF16), pl.BlockSpec((D // 4, C), lambda j, s: (0, j)))] * 4,
        [pltpu.VMEM((T, C), BF16)], "chunks_back", 5 * MATMUL * count * C // F,
        aliases={7: 0, 8: 1, 9: 2} if filled else None,
    )


def kept_rows(scalars, a, dg, du):
    def kernel(s, dg_ref, du_ref, a0, a1, *outs):
        sent_rows((a0, a1), dg_ref, du_ref, outs)

    return call(
        kernel, scalars, F // C,
        [(t, pl.BlockSpec((T, C), lambda j, s: (0, j))) for t in (dg, du)] + [columns_of(a, PARTNER), columns_of(a, ME)],
        [(shape((D // 4, F), BF16), pl.BlockSpec((D // 4, C), lambda j, s: (0, j)))] * 4,
        [], "kept_rows", MATMUL,
    )


def states_back(scalars, h, dh, dg, du, wg, wu, layer):
    def kernel(s, h_ref, dh_ref, dg_ref, du_ref, g_ref, u_ref, out, total):
        j = pl.program_id(0)

        def body(t):
            part = nt(dg_ref[t, :], g_ref[0]) + nt(du_ref[t, :], u_ref[0])

            @pl.when(j == 0)
            def _():
                total[t, :] = part

            @pl.when(j > 0)
            def _():
                total[t, :] += part

            @pl.when(j == F // C - 1)
            def _():
                out[t, :] = dh_ref[t, :] + norm_back(h_ref[t, :], total[t, :])

        over_tokens(body)

    return call(
        kernel, scalars, F // C,
        [(h, whole((T, D))), (dh, whole((T, D)))]
        + [(t, pl.BlockSpec((T, C), lambda j, s: (0, j))) for t in (dg, du)]
        + [(w, pl.BlockSpec((1, D, C), lambda j, s: (layer, 0, j))) for w in (wg, wu)],
        [(shape((T, D), BF16), whole((T, D)))],
        [pltpu.VMEM((T, D), F32)], "states_back", 2 * MATMUL,
    )[0]


def update(scalars, own, near, far, w, m, v, layer, filled=None):
    rows, cols = own.shape
    split = len(far) == 2
    if split:
        block = (rows, C)
        here = pl.BlockSpec(block, lambda j, s: (0, s[OTHERS + j]))
        fars = [pl.BlockSpec(block, lambda j, s: (0, jnp.minimum(j, 2))), pl.BlockSpec(block, lambda j, s: (0, jnp.maximum(j - 3, 0)))]
        mine = pl.BlockSpec((1,) + block, lambda j, s: (layer, 0, s[OTHERS + j]))
        stacked = pl.BlockSpec((1,) + block, lambda j, s: (layer, s[ME], s[OTHERS + j]))
    else:
        block = (rows // 5, cols)
        here = pl.BlockSpec(block, lambda j, s: (j, 0))
        fars = [here]
        mine = pl.BlockSpec((1,) + block, lambda j, s: (layer, j, 0))
        stacked = pl.BlockSpec((1,) + block, lambda j, s: (layer, s[ME] * 5 + j, 0))

    def kernel(s, own_ref, near_ref, *refs):
        far_refs, refs = refs[: len(far)], refs[len(far) :]
        w_ref, m_ref, v_ref, *refs = refs
        ws_out, m_out, v_out, new_out = refs[3:] if filled else refs
        there = far_refs[0][...].astype(F32)
        if split:
            there = jnp.where(pl.program_id(0) < 3, there, far_refs[1][...].astype(F32))
        g = (own_ref[...].astype(F32) + near_ref[...].astype(F32) + there).astype(BF16).astype(F32)
        wide = w_ref[0].astype(F32)
        m = 0.9 * m_ref[0] + 0.1 * g
        v = 0.95 * v_ref[0] + 0.05 * g * g
        new = (wide - 0.02 * (m * lax.rsqrt(v + 1e-8) + 0.1 * wide)).astype(BF16)
        m_out[0], v_out[0], ws_out[0] = m, v, new
        new_out[...] = new

    n = 5 + len(far)
    return call(
        kernel, scalars, 5,
        [(own, here), (near, here)] + list(zip(far, fars)) + [(w, stacked), (m, mine), (v, mine)] + [(t, ANY) for t in filled or ()],
        [(shape(w.shape, BF16), stacked)] + [(shape(m.shape, F32), mine)] * 2 + [(shape((rows, cols), BF16), here)],
        [], "update", rows * cols * 20, aliases={n: 0, n + 1: 1, n + 2: 2} if filled else None,
    )


def solution(mesh):
    def body(x, dy, wg, wu, wd, mg, mu, md, vg, vu, vd):
        me = lax.axis_index("dp")
        partner, across, diagonal = me ^ 1, me ^ 2, me ^ 3
        orders = jnp.array([[4, 3, 2, 1, 0], [0, 1, 2, 3, 4]], jnp.int32)
        chip = me // 2
        places = jnp.stack([me, partner, across, diagonal]).astype(jnp.int32)
        scalars = jnp.concatenate([places, orders[chip], orders[1 - chip]])
        h0, dy = x[0], dy[0]
        last = [h0]

        def tie(*arrays):
            *arrays, _ = lax.optimization_barrier((*arrays, last[0]))
            return arrays[0] if len(arrays) == 1 else arrays

        def done(array):
            last[0] = array

        def block(t, which, rows):
            return lax.dynamic_slice_in_dim(t, which * rows, rows, 0)

        def cores(t):
            return lax.ppermute(t, "dp", CORES)

        def chips(t):
            return lax.ppermute(t, "dp", CHIPS)

        def across_chips(theirs, got):
            theirs, got = tie(theirs, got)
            total = (theirs.astype(F32) + got.astype(F32)).astype(BF16)
            done(total)
            return chips(total)

        def spread(new):
            near, far = cores(new), chips(new)
            return near, far

        def place(out, layer, blocks, who):
            rows = blocks[0].shape[0]
            blocks = tie(*blocks) if len(blocks) > 1 else [tie(blocks[0])]
            for b, w in zip(blocks, who):
                out = lax.dynamic_update_slice(out, b[None], (layer, w * rows, 0))
            done(out)
            return out

        quarter = F // 4
        a0, h1 = forward(scalars, h0, wg, wu, wd, 0)
        a1, gate, up, gd1 = first_down(scalars, h1, dy, wg, wu, 1, 0, 3)
        got = cores(block(gd1, diagonal, quarter))
        done(gd1)
        far_d1 = across_chips(block(gd1, across, quarter), got)

        dg, du, g_diag, g_theirs, u_diag, u_theirs = first_back(scalars, tie(a1), dy, gate, up, wd, 1, 0, 3)
        done(dg)
        got_g, got_u = cores(g_diag), cores(u_diag)
        far_ga = across_chips(g_theirs, got_g)
        far_ua = across_chips(u_theirs, got_u)

        dg, du, gd1, g_diag, g_theirs, u_diag, u_theirs = chunks_back(scalars, tie(a1), dy, wg, wu, wd, 1, 3, 2, (dg, du, gd1))
        got_g, got_u = cores(g_diag), cores(u_diag)
        near_d1 = cores(block(gd1, partner, quarter))
        own_d1 = block(gd1, me, quarter)
        done(dg)
        gp, go, up_, uo = kept_rows(scalars, tie(a1), dg, du)
        near_g1, near_u1 = cores(gp), cores(up_)
        done(go)
        far_gb = across_chips(g_theirs, got_g)
        far_ub = across_chips(u_theirs, got_u)

        dh1 = states_back(scalars, tie(h1), dy, dg, du, wg, wu, 1)
        done(dh1)
        stack_d = update(scalars, tie(own_d1), near_d1, (far_d1,), wd, md, vd, 1)
        done(stack_d[3])
        sent_d1 = spread(stack_d[3])
        stack_g = update(scalars, tie(go), near_g1, (far_ga, far_gb), wg, mg, vg, 1)
        done(stack_g[3])
        sent_g1 = spread(stack_g[3])
        stack_u = update(scalars, tie(uo), near_u1, (far_ua, far_ub), wu, mu, vu, 1)
        done(stack_u[3])
        sent_u1 = spread(stack_u[3])

        dg, du, gd0, g_diag, g_theirs, u_diag, u_theirs = chunks_back(scalars, tie(a0), dh1, wg, wu, wd, 0, 0, 3)
        done(dg)
        got_d = cores(block(gd0, diagonal, quarter))
        got_g, got_u = cores(g_diag), cores(u_diag)
        theirs_d = block(gd0, across, quarter)
        relay_d1 = cores(tie(sent_d1[1]))
        far_d0 = across_chips(theirs_d, got_d)
        far_ga = across_chips(g_theirs, got_g)
        far_ua = across_chips(u_theirs, got_u)
        dg, du, gd0, g_diag, g_theirs, u_diag, u_theirs = chunks_back(scalars, tie(a0), dh1, wg, wu, wd, 0, 3, 2, (dg, du, gd0))
        got_g, got_u = cores(g_diag), cores(u_diag)
        near_d0 = cores(block(gd0, partner, quarter))
        own_d0 = block(gd0, me, quarter)
        done(dg)
        gp, go, up_, uo = kept_rows(scalars, tie(a0), dg, du)
        near_g0, near_u0 = cores(gp), cores(up_)
        done(go)
        far_gb = across_chips(g_theirs, got_g)
        far_ub = across_chips(u_theirs, got_u)

        out_d = place(stack_d[0], 1, [sent_d1[0], sent_d1[1]], [partner, across])
        relay_g1 = cores(tie(sent_g1[1]))
        out_g = place(stack_g[0], 1, [sent_g1[0], sent_g1[1]], [partner, across])
        out_d = place(out_d, 1, [relay_d1], [diagonal])
        relay_u1 = cores(tie(sent_u1[1]))
        out_u = place(stack_u[0], 1, [sent_u1[0], sent_u1[1]], [partner, across])
        out_g = place(out_g, 1, [relay_g1], [diagonal])
        out_u = place(out_u, 1, [relay_u1], [diagonal])

        out_d, m_d, v_d, new = update(scalars, tie(own_d0), near_d0, (far_d0,), wd, md, vd, 0, (out_d, *stack_d[1:3]))
        done(new)
        sent_d0 = spread(new)
        out_g, m_g, v_g, new = update(scalars, tie(go), near_g0, (far_ga, far_gb), wg, mg, vg, 0, (out_g, *stack_g[1:3]))
        done(new)
        sent_g0 = spread(new)
        out_u, m_u, v_u, new = update(scalars, tie(uo), near_u0, (far_ua, far_ub), wu, mu, vu, 0, (out_u, *stack_u[1:3]))
        done(new)
        sent_u0 = spread(new)
        out_d = place(out_d, 0, [sent_d0[0]], [partner])
        out_g = place(out_g, 0, [sent_g0[0]], [partner])
        out_u = place(out_u, 0, [sent_u0[0]], [partner])
        relay_d0 = cores(tie(sent_d0[1]))
        out_d = place(out_d, 0, [sent_d0[1]], [across])
        out_d = place(out_d, 0, [relay_d0], [diagonal])
        relay_g0 = cores(tie(sent_g0[1]))
        out_g = place(out_g, 0, [sent_g0[1]], [across])
        out_g = place(out_g, 0, [relay_g0], [diagonal])
        relay_u0 = cores(tie(sent_u0[1]))
        out_u = place(out_u, 0, [sent_u0[1]], [across])
        out_u = place(out_u, 0, [relay_u0], [diagonal])
        return out_g, out_u, out_d, m_g, m_u, m_d, v_g, v_u, v_d

    both = P(("rep", "dp"))
    part = P(None, "dp")
    return jax.shard_map(
        body, mesh=mesh,
        in_specs=(both, both, P(), P(), P(), part, part, part, part, part, part),
        out_specs=(P("rep"),) * 3 + (P("rep", "dp"),) * 6,
        check_vma=False,
    )
```
